32 devices in a mesh: row: 2 (over y), col: 4 (over x, core), rep: 4 (over z).
Axes of the slice: x: 2, y: 2, z: 4, core: 2. Of those that a mesh axis runs over, the one named last changes fastest.
Arguments:
- hidden: bfloat16 [512, 7168], P('rep'), may hold values from -6 to 6
- train_weight: bfloat16 [7168, 16384], P(('rep', 'row'), 'col'), may hold values from -0.0625 to 0.0625
- shard_order: int32 [4, 4, 2], replicated, may hold values from 0 to 1, each once within a row
Outputs:
- served_weight: bfloat16 [7168, 16384], P(None, ('col', 'row'))
- projected: float32 [512, 16384], P('rep', ('col', 'row'))
The draws below stay inside these ranges and needn't reach their ends.
Inputs may be any that keep to these rules, and one draw needn't show every extreme that they name: Each shard_order[c, k] is a permutation of 0 to 1.
All inputs are finite; a program needn't handle non-finite values.
Results may differ from the reference program's by a relative error of at most 0.001.
Values may be sent and summed in bfloat16 or wider, within the bound.
No kernel may reach another device: no remote copies, remote signals or barrier semaphores. Data moves between devices by JAX's collectives and lax.ppermute only.
A program may use at most 128 MiB of HBM per device.

```python
import jax
import jax.numpy as jnp

D = 7168
F = 16384
SUB_BLOCKS = 4
SEQS = 512
N_ROW = 2
N_COL = 4


def block_scale(rng, shape, cuts, least, high):
    def one(dim, shards_of):
        heights = jax.random.uniform(jax.random.fold_in(jax.random.fold_in(rng, 6), dim), (shards_of,), jnp.float32, least / len(cuts), high / len(cuts))
        return jnp.repeat(jnp.exp(heights), shape[dim] // shards_of).reshape((-1,) + (1,) * (len(shape) - dim - 1))

    loudness = one(*cuts[0])
    for cut in cuts[1:]:
        loudness = loudness * one(*cut)
    return loudness


def centred(key, extent, width, reach, split=(), dtype=jnp.bfloat16):
    drawn = width * jax.random.normal(key, extent, jnp.float32)
    if split:
        drawn = drawn * block_scale(key, extent, split, -0.22, 0.18)
    return jnp.clip(drawn, -reach, reach).astype(dtype)


def setup_inputs(seed: int = 0) -> dict:
    arg_keys = jax.random.split(jax.random.key(seed), 4)
    hidden = centred(arg_keys[0], (SEQS, D), 1.0, 6.0, ((0, 4),))
    train_weight = centred(arg_keys[1], (D, F), D ** -0.5, 0.0625, ((0, 8), (1, 4)))
    shard_order = jax.vmap(lambda own: jax.random.permutation(own, N_ROW))(jax.random.split(arg_keys[2], N_COL * SUB_BLOCKS)).reshape((N_COL, SUB_BLOCKS, N_ROW)).astype(jnp.int32)
    return dict(hidden=hidden, train_weight=train_weight, shard_order=shard_order)


def reference(hidden, train_weight, shard_order):
    block_cols = F // (N_ROW * N_COL)
    sub_cols = block_cols // SUB_BLOCKS
    blocks = train_weight.reshape(D, N_COL, N_ROW, SUB_BLOCKS, sub_cols)
    order = shard_order.astype(jnp.int32)
    pieces = []
    for index in range(SUB_BLOCKS):
        subset = blocks[:, :, :, index, :]
        picks = jnp.broadcast_to(order[:, index, :][None, :, :, None], subset.shape)
        pieces.append(jnp.take_along_axis(subset, picks, axis=2))
    served = jnp.stack(pieces, axis=3).reshape(D, F)
    projected = jnp.dot(hidden, served, preferred_element_type=jnp.float32)
    return served, projected
```

```python
from collections import deque

import jax
import jax.numpy as jnp
from jax import lax
from jax.experimental import pallas as pl
from jax.sharding import PartitionSpec as P

CHUNK_BYTES = 1 << 19


def unwritten(shape, dtype):
    return pl.pallas_call(
        lambda out: None,
        out_shape=jax.ShapeDtypeStruct(shape, dtype),
        out_specs=pl.BlockSpec(memory_space=pl.ANY),
    )()


def shards(hidden, train_weight, shard_order):
    row_count = lax.axis_size("row")
    rep_count = lax.axis_size("rep")
    row = lax.axis_index("row")
    rep = lax.axis_index("rep")
    rows_tile, cols_tile = train_weight.shape
    piece_cols = cols_tile // row_count
    sub_count = shard_order.shape[1]
    sub_cols = piece_cols // sub_count
    my_order = lax.dynamic_index_in_dim(shard_order, lax.axis_index("col"), 0, keepdims=False)
    chunks = sub_count
    while chunks > 1 and rows_tile * piece_cols * 2 // chunks < CHUNK_BYTES:
        chunks //= 2
    subs_per = sub_count // chunks
    chunk_cols = sub_cols * subs_per

    def pick(chunk, target):
        order = lax.dynamic_index_in_dim(my_order, target, 1, keepdims=False)
        subs = []
        for sub in range(chunk * subs_per, (chunk + 1) * subs_per):
            start = order[sub] * piece_cols + sub * sub_cols
            subs.append(lax.dynamic_slice(train_weight, (0, start), (rows_tile, sub_cols)))
        return jnp.concatenate(subs, axis=1) if len(subs) > 1 else subs[0]

    ring = [(i, (i + 1) % rep_count) for i in range(rep_count)]
    served = unwritten((row_count * rep_count * rows_tile, piece_cols), train_weight.dtype)
    totals = [jnp.zeros((hidden.shape[0], chunk_cols), jnp.float32) for _ in range(chunks)]

    def land(data, sources, chunk, hops):
        nonlocal served
        origin = lax.rem(rep + rep_count - hops, rep_count)
        for block, source in zip(data, sources):
            at = (origin * row_count + source) * rows_tile
            served = lax.dynamic_update_slice(served, block, (at, chunk * chunk_cols))
            features = lax.dynamic_slice(hidden, (0, at), (hidden.shape[0], rows_tile))
            totals[chunk] = totals[chunk] + jnp.dot(features, block, preferred_element_type=jnp.float32)

    def hop(data):
        return [lax.ppermute(block, "rep", ring) for block in data]

    flight = deque()
    for chunk in range(chunks):
        own = [pick(chunk, row)]
        flight.append((hop(own), [row], chunk, 1))
        land(own, [row], chunk, 0)
    shifts = range(1, row_count)
    for chunk in range(chunks):
        swapped = [
            lax.ppermute(
                pick(chunk, lax.rem(row + shift, row_count)),
                "row",
                [(i, (i + shift) % row_count) for i in range(row_count)],
            )
            for shift in shifts
        ]
        sources = [lax.rem(row + row_count - shift, row_count) for shift in shifts]
        flight.append((hop(swapped), sources, chunk, 1))
        land(swapped, sources, chunk, 0)
    while flight:
        data, sources, chunk, hops = flight.popleft()
        if hops + 1 < rep_count:
            flight.append((hop(data), sources, chunk, hops + 1))
        land(data, sources, chunk, hops)
    return (served, jnp.concatenate(totals, axis=1))


def solution(mesh):
    placed = (P("rep", None), P(("rep", "row"), "col"), P())
    return jax.shard_map(
        shards,
        mesh=mesh,
        in_specs=placed,
        out_specs=(P(None, ("col", "row")), P("rep", ("col", "row"))),
        check_vma=False,
    )
```

```python
from collections import deque

import jax
import jax.numpy as jnp
from jax import lax
from jax.experimental import pallas as pl
from jax.sharding import PartitionSpec as P

CHUNK_BYTES = 1 << 19


def unwritten(shape, dtype):
    return pl.pallas_call(
        lambda out: None,
        out_shape=jax.ShapeDtypeStruct(shape, dtype),
        out_specs=pl.BlockSpec(memory_space=pl.ANY),
    )()


def chunk_count(rows_tile, piece_cols, sub_count):
    chunks = sub_count
    while chunks > 1 and rows_tile * piece_cols * 2 // chunks < CHUNK_BYTES:
        chunks //= 2
    return chunks


def shards(hidden, train_weight, shard_order):
    row_count = lax.axis_size("row")
    rep_count = lax.axis_size("rep")
    row = lax.axis_index("row")
    rep = lax.axis_index("rep")
    col = lax.axis_index("col")
    rows_tile, cols_tile = train_weight.shape
    piece_cols = cols_tile // row_count
    sub_count = shard_order.shape[1]
    sub_cols = piece_cols // sub_count
    chunks = chunk_count(rows_tile, piece_cols, sub_count)
    subs_per = sub_count // chunks
    chunk_cols = sub_cols * subs_per

    def cut(array, starts, sizes):
        return lax.dynamic_slice(array, starts, sizes, allow_negative_indices=False)

    last_pick = None

    def pick(chunk, target):
        nonlocal last_pick
        subs = []
        for sub in range(chunk * subs_per, (chunk + 1) * subs_per):
            block = cut(shard_order, (col, sub, target), (1, 1, 1)).reshape(())
            start = block * piece_cols + sub * sub_cols
            if last_pick is not None:
                start, _ = lax.optimization_barrier((start, last_pick))
            subs.append(cut(train_weight, (0, start), (rows_tile, sub_cols)))
        picked = jnp.concatenate(subs, axis=1) if len(subs) > 1 else subs[0]
        last_pick = lax.optimization_barrier(picked)
        return last_pick

    ring = [(i, (i + 1) % rep_count) for i in range(rep_count)]
    served = unwritten((row_count * rep_count * rows_tile, piece_cols), train_weight.dtype)
    totals = [None] * chunks

    def land(data, sources, chunk, hops):
        nonlocal served
        origin = lax.rem(rep + rep_count - hops, rep_count)
        for block, source in zip(data, sources):
            at = (origin * row_count + source) * rows_tile
            served = lax.dynamic_update_slice(
                served, block, (at, chunk * chunk_cols), allow_negative_indices=False
            )
            features = cut(hidden, (0, at), (hidden.shape[0], rows_tile))
            part = jnp.dot(features, block, preferred_element_type=jnp.float32)
            totals[chunk] = part if totals[chunk] is None else totals[chunk] + part

    def hop(data):
        return [lax.ppermute(block, "rep", ring) for block in data]

    flight = deque()
    owns = []
    for chunk in range(chunks):
        own = [pick(chunk, row)]
        owns.append(own)
        flight.append((hop(own), [row], chunk, 1, "o"))
    shifts = range(1, row_count)
    swaps = []
    for chunk in range(chunks):
        swapped = []
        for shift in shifts:
            block = pick(chunk, lax.rem(row + shift, row_count))
            swapped.append(
                lax.ppermute(block, "row", [(i, (i + shift) % row_count) for i in range(row_count)])
            )
        sources = [lax.rem(row + row_count - shift, row_count) for shift in shifts]
        swaps.append((swapped, sources))
        flight.append((hop(swapped), sources, chunk, 1, "s"))
    for chunk in range(chunks):
        land(owns[chunk], [row], chunk, 0)
    for chunk, (swapped, sources) in enumerate(swaps):
        land(swapped, sources, chunk, 0)
    while flight:
        data, sources, chunk, hops, tag = flight.popleft()
        if hops + 1 < rep_count:
            flight.append((hop(data), sources, chunk, hops + 1, tag))
        land(data, sources, chunk, hops)
    return (served, jnp.concatenate(totals, axis=1))


def solution(mesh):
    placed = (P("rep", None), P(("rep", "row"), "col"), P())

    return jax.shard_map(
        shards,
        mesh=mesh,
        in_specs=placed,
        out_specs=(P(None, ("col", "row")), P("rep", ("col", "row"))),
        check_vma=False,
    )
```

```python
from collections import deque

import jax
import jax.numpy as jnp
from jax import lax
from jax.experimental import pallas as pl
from jax.sharding import PartitionSpec as P

CHUNK_BYTES = 1 << 19


def unwritten(shape, dtype):
    return pl.pallas_call(
        lambda out: None,
        out_shape=jax.ShapeDtypeStruct(shape, dtype),
        out_specs=pl.BlockSpec(memory_space=pl.ANY),
    )()


def chunk_count(rows_tile, piece_cols, sub_count):
    chunks = sub_count
    while chunks > 1 and rows_tile * piece_cols * 2 // chunks < CHUNK_BYTES:
        chunks //= 2
    return chunks


def shards(hidden, train_weight, shard_order):
    row_count = lax.axis_size("row")
    rep_count = lax.axis_size("rep")
    row = lax.axis_index("row")
    rep = lax.axis_index("rep")
    col = lax.axis_index("col")
    rows_tile, cols_tile = train_weight.shape
    piece_cols = cols_tile // row_count
    sub_count = shard_order.shape[1]
    sub_cols = piece_cols // sub_count
    chunks = chunk_count(rows_tile, piece_cols, sub_count)
    subs_per = sub_count // chunks
    chunk_cols = sub_cols * subs_per

    def cut(array, starts, sizes):
        return lax.dynamic_slice(array, starts, sizes, allow_negative_indices=False)

    last_pick = None
    group = col

    def pick(chunk, target):
        nonlocal last_pick, group
        subs = []
        for sub in range(chunk * subs_per, (chunk + 1) * subs_per):
            block = cut(shard_order, (group, sub, target), (1, 1, 1)).reshape(())
            start = block * piece_cols + sub * sub_cols
            if last_pick is not None:
                start, _ = lax.optimization_barrier((start, last_pick))
            subs.append(cut(train_weight, (0, start), (rows_tile, sub_cols)))
        picked = jnp.concatenate(subs, axis=1) if len(subs) > 1 else subs[0]
        if last_pick is None:
            group, last_pick = lax.optimization_barrier((col, picked))
        else:
            last_pick = lax.optimization_barrier(picked)
        return last_pick

    ring = [(i, (i + 1) % rep_count) for i in range(rep_count)]
    served = unwritten((row_count * rep_count * rows_tile, piece_cols), train_weight.dtype)
    totals = [None] * chunks

    def land(data, sources, chunk, hops, place=True, multiply=True):
        nonlocal served
        origin = lax.rem(rep + rep_count - hops, rep_count)
        for block, source in zip(data, sources):
            at = (origin * row_count + source) * rows_tile
            if multiply:
                features = cut(hidden, (0, at), (hidden.shape[0], rows_tile))
                part = jnp.dot(features, block, preferred_element_type=jnp.float32)
                totals[chunk] = part if totals[chunk] is None else totals[chunk] + part
            if place:
                served = lax.dynamic_update_slice(served, block, (at, chunk * chunk_cols), allow_negative_indices=False)

    def hop(data):
        return [lax.ppermute(block, "rep", ring) for block in data]

    flight = deque()
    owns = []
    for chunk in range(chunks):
        own = [pick(chunk, row)]
        owns.append(own)
        flight.append((hop(own), [row], chunk, 1, "o"))
    shifts = range(1, row_count)
    swaps = []
    for chunk in range(chunks):
        swapped = []
        for shift in shifts:
            block = pick(chunk, lax.rem(row + shift, row_count))
            swapped.append(
                lax.ppermute(block, "row", [(i, (i + shift) % row_count) for i in range(row_count)])
            )
        sources = [lax.rem(row + row_count - shift, row_count) for shift in shifts]
        swaps.append((swapped, sources))
        flight.append((hop(swapped), sources, chunk, 1, "s"))
    for chunk in range(chunks):
        land(owns[chunk], [row], chunk, 0)
    for chunk, (swapped, sources) in enumerate(swaps):
        land(swapped, sources, chunk, 0)
    while flight:
        data, sources, chunk, hops, tag = flight.popleft()
        if hops + 1 < rep_count:
            flight.append((hop(data), sources, chunk, hops + 1, tag))
        land(data, sources, chunk, hops, place=bool(flight))
    early = totals[:-1] + [jnp.zeros_like(totals[-1])]
    joined = lax.optimization_barrier(jnp.concatenate(early, axis=1))
    projected = lax.dynamic_update_slice(joined, totals[-1], (0, (chunks - 1) * chunk_cols))
    projected, data = lax.optimization_barrier((projected, data))
    land(data, sources, chunk, hops, multiply=False)
    return (served, projected)


def solution(mesh):
    placed = (P("rep", None), P(("rep", "row"), "col"), P())

    return jax.shard_map(
        shards,
        mesh=mesh,
        in_specs=placed,
        out_specs=(P(None, ("col", "row")), P("rep", ("col", "row"))),
        check_vma=False,
    )
```
